32 devices in a mesh: dp: 4 (over z), vocab: 8 (over y, x, core).
Axes of the slice: x: 2, y: 2, z: 4, core: 2. Of those that a mesh axis runs over, the one named last changes fastest.
Arguments:
- hidden: bfloat16 [3072, 896], P(('dp', 'vocab')), may hold values from -400 to 400
- target_ids: int32 [3072], P('dp'), may hold values from 0 to 151935
- owner: int32 [4, 24], P('dp'), may hold values from 0 to 23, each once within a row
- head: bfloat16 [896, 151936], P(None, 'vocab'), may hold values from -0.1875 to 0.1875
Outputs:
- owned_loss: float32 [96, 32], P(('dp', 'vocab'))
The draws below stay inside these ranges and needn't reach their ends.
Inputs may be any that keep to these rules, and one draw needn't show every extreme that they name: Each row of owner names every slot once.
All inputs are finite; a program needn't handle non-finite values.
Results may differ from the reference program's by a relative error of at most 0.0003.
Values may be sent and summed in bfloat16 or wider, within the bound.
No kernel may reach another device: no remote copies, remote signals or barrier semaphores. Data moves between devices by JAX's collectives and lax.ppermute only.
A program may use at most 128 MiB of HBM per device.

```python
import math
import jax
import jax.numpy as jnp
import numpy as np
from jax import lax

D = 896
V = 151936
LEN = 32
SEQ_G = 24
TOKENS = 3072
N_DP = 4


def draw_hidden(key, part):
    key_rows, key_scale = jax.random.split(jax.random.fold_in(key, 11), 2)
    noise = jnp.clip(jax.random.normal(key_rows, (TOKENS, D), jnp.float32), -6.0, 6.0)
    scales = 1.5 * jnp.exp(jax.random.uniform(key_scale, (TOKENS, 1), jnp.float32, 0.0, jnp.log(8.0)))
    values = scales * noise
    return jnp.clip(values, -400.0, 400.0).astype(jnp.bfloat16)


def place_ends(result, key, least, largest):
    shape = result.shape
    place = [jax.random.randint(jax.random.fold_in(key, axis), (), 0, shape[axis]) for axis in range(len(shape))]
    result = result.at[tuple(place)].set(least)
    longest = shape.index(max(shape))
    place[longest] = (place[longest] + 1) % shape[longest]
    return result.at[tuple(place)].set(largest)


def shard_levels(stream_key, extent, cuts, least, high):
    gain, own = 1.0, jax.random.fold_in(stream_key, 6)
    for axis_at, blocks in cuts:
        steps = jnp.exp(jax.random.uniform(jax.random.fold_in(own, axis_at), (blocks,), jnp.float32, least / len(cuts), high / len(cuts)))
        gain = gain * jnp.repeat(steps, extent[axis_at] // blocks).reshape([-1 if axis == axis_at else 1 for axis in range(len(extent))])
    return gain


def wide_ids(own_key, extent, amount, slope):
    portions = [min(1 << octave, amount + 1 - (1 << octave)) * (1 << 20) // math.isqrt((1 << octave) ** slope) + 1 for octave in range((amount + 1).bit_length()) if 1 << octave <= amount]
    deviation = 1 + sum(portions) // (1 << 30)
    listing = np.cumsum(np.array([max(1, weight // deviation) for weight in portions]))
    ticket = jax.random.randint(jax.random.fold_in(own_key, 1), extent, 0, int(listing[len(portions) - 1]))
    start = jnp.left_shift(1, jnp.searchsorted(jnp.asarray(listing, jnp.int32), ticket, side="right").astype(jnp.int32))
    rank = start - 1 + jax.random.randint(jax.random.fold_in(own_key, 4), extent, 0, 1 << 30) % jnp.minimum(start, amount + 1 - start)
    return jax.random.permutation(jax.random.fold_in(own_key, 2), amount)[rank].astype(jnp.int32)


def scatter_about(own_key, dims, scale, bound, shards=(), kind=jnp.bfloat16):
    entries = jax.random.normal(own_key, dims, jnp.float32) * scale
    if len(shards) > 0:
        entries = shard_levels(own_key, dims, shards, -0.22, 0.18) * entries
    return jnp.clip(entries, min=-bound, max=bound).astype(kind)


def setup_inputs(seed: int = 0) -> dict:
    streams_of = jax.random.split(jax.random.key(seed), 5)
    return {
        "hidden": draw_hidden(jax.random.fold_in(streams_of[4], 71), 0),
        "target_ids": place_ends(wide_ids(streams_of[1], (TOKENS,), V, 2), jax.random.fold_in(streams_of[1], 3), 0, V - 1).astype(jnp.int32),
        "owner": jax.vmap(lambda own: jax.random.permutation(own, SEQ_G))(jax.random.split(streams_of[2], N_DP)).reshape((N_DP, SEQ_G)).astype(jnp.int32),
        "head": scatter_about(streams_of[3], (D, V), D ** -0.5, 0.1875, ((1, 8),)),
    }


def token_losses(rows, labels, head):
    logits = jnp.dot(rows, head, preferred_element_type=jnp.float32)
    peak = jnp.max(logits, axis=1)
    expsum = jnp.sum(jnp.exp(logits - peak[:, None]), axis=1)
    column = lax.broadcasted_iota(jnp.int32, logits.shape, 1)
    picked = jnp.sum(jnp.where(column == labels.astype(jnp.int32)[:, None], logits, jnp.zeros_like(logits)), axis=1)
    return peak + jnp.log(expsum) - picked


def reference(hidden, target_ids, owner, head):
    count = hidden.shape[0]
    step_rows = math.gcd(count, 512)
    blocks = (hidden.reshape(count // step_rows, step_rows, hidden.shape[1]), target_ids.reshape(count // step_rows, step_rows))
    losses = lax.map(lambda pair: token_losses(pair[0], pair[1], head), blocks)
    losses = losses.reshape(N_DP, SEQ_G, LEN)
    groups = jnp.arange(N_DP, dtype=jnp.int32)[:, None]
    placed = jnp.zeros_like(losses).at[groups, owner.astype(jnp.int32)].set(losses)
    return placed.reshape(N_DP * SEQ_G, LEN)
```

```python
import functools
import math

import jax
import jax.numpy as jnp
from jax import lax
from jax.experimental import pallas as pl
from jax.experimental.pallas import tpu as pltpu
from jax.sharding import PartitionSpec as P

LOG2E = math.log2(math.e)
FLOOR = -1e30


def tree(op, values):
    while len(values) > 1:
        paired = [op(a, b) for a, b in zip(values[::2], values[1::2])]
        values = paired + ([values[-1]] if len(values) % 2 else [])
    return values[0]


def head_kernel(x_ref, lab_ref, w_ref, o_ref, m_ref, s_ref, p_ref, lb_ref, xt_ref, *, chunk, width, group):
    tokens = x_ref.shape[0]
    block = w_ref.shape[0]
    step, steps = pl.program_id(0), pl.num_programs(0)

    @pl.when(step == 0)
    def _():
        labels = lab_ref[...]
        labels = jnp.where((labels >= 0) & (labels < width), labels, -(1 << 30))
        lb_ref[...] = jnp.broadcast_to(labels, lb_ref.shape)
        m_ref[...] = jnp.full_like(m_ref, FLOOR)
        s_ref[...] = jnp.zeros_like(s_ref)
        p_ref[...] = jnp.zeros_like(p_ref)
        xt_ref[...] = x_ref[...].T

    sub = lax.broadcasted_iota(jnp.int32, (8, 128), 0)

    def run(masked):
        for r0 in range(0, block, chunk):
            logits = jnp.dot(w_ref[r0 : r0 + chunk, :], xt_ref[...], preferred_element_type=jnp.float32)
            for c in range(tokens // 128):
                cols = slice(c * 128, (c + 1) * 128)
                label, pick, top, total = lb_ref[:, cols], p_ref[:, cols], m_ref[:, cols], s_ref[:, cols]
                for g in range(0, chunk, group):
                    scaled = []
                    for r in range(g, min(g + group, chunk), 8):
                        value = logits[r : r + 8, cols]
                        row = sub + (step * block + r0 + r)
                        pick = jnp.where(label == row, value, pick)
                        value = value * LOG2E
                        if masked:
                            value = jnp.where(row < width, value, FLOOR)
                        scaled.append(value)
                    peak = jnp.maximum(top, tree(jnp.maximum, scaled))
                    total = total * jnp.exp2(top - peak) + tree(jnp.add, [jnp.exp2(v - peak) for v in scaled])
                    top = peak
                p_ref[:, cols], m_ref[:, cols], s_ref[:, cols] = pick, top, total

    @pl.when(step < steps - 1)
    def _():
        run(False)

    @pl.when(step == steps - 1)
    def _():
        run(width % block != 0)
        top = m_ref[...]
        peak = jnp.max(top, axis=0, keepdims=True)
        total = jnp.sum(s_ref[...] * jnp.exp2(top - peak), axis=0, keepdims=True)
        o_ref[0:1, :] = (peak + jnp.log2(total)) * (1.0 / LOG2E)
        o_ref[1:2, :] = jnp.sum(p_ref[...], axis=0, keepdims=True)


def head_stats(x, labels, rows):
    tokens, depth = x.shape
    width = rows.shape[0]
    block, chunk = 1920, 192
    return pl.pallas_call(
        functools.partial(head_kernel, chunk=chunk, width=width, group=48),
        out_shape=jax.ShapeDtypeStruct((2, tokens), jnp.float32),
        grid=(pl.cdiv(width, block),),
        in_specs=[
            pl.BlockSpec((tokens, depth), lambda j: (0, 0)),
            pl.BlockSpec((1, tokens), lambda j: (0, 0)),
            pl.BlockSpec((block, depth), lambda j: (j, 0)),
        ],
        out_specs=pl.BlockSpec((2, tokens), lambda j: (0, 0)),
        scratch_shapes=[pltpu.VMEM((8, tokens), jnp.float32)] * 3
        + [pltpu.VMEM((8, tokens), jnp.int32), pltpu.VMEM((depth, tokens), x.dtype)],
        compiler_params=pltpu.CompilerParams(vmem_limit_bytes=60 << 20),
    )(x, labels, rows)


def local(hidden, target_ids, owner, head):
    shards, me = lax.axis_size("vocab"), lax.axis_index("vocab")
    width = head.shape[1]
    count = hidden.shape[0]
    seq_group = owner.shape[1]
    own_count = seq_group // shards
    length = target_ids.shape[0] // seq_group

    def swap(v, k):
        return lax.ppermute(v, "vocab", [(i, i ^ k) for i in range(shards)])

    places = list(range(0, shards, 2)) + list(range(1, shards, 2))
    even = [hidden] + [swap(hidden, k) for k in range(2, shards, 2)]
    x = jnp.concatenate(even + [swap(v, 1) for v in even], 0)
    labels = jnp.concatenate([lax.dynamic_slice_in_dim(target_ids, (me ^ k) * count, count) for k in places])
    stats = head_stats(x, (labels - me * width)[None, :], head.T)

    per_shard = count // length
    slots = jnp.concatenate([lax.dynamic_slice_in_dim(owner[0], (me ^ k) * per_shard, per_shard) for k in places])
    onehot = (lax.broadcasted_iota(jnp.int32, (seq_group, seq_group), 0) == slots[None, :]).astype(jnp.float32)
    by_seq = stats.reshape(2, seq_group, length).transpose(1, 0, 2).reshape(seq_group, 2 * length)
    send = jnp.dot(onehot, by_seq, precision=lax.Precision.HIGHEST)
    got = lax.all_to_all(send, "vocab", split_axis=0, concat_axis=0, tiled=True)
    got = got.reshape(shards, own_count, 2, length)
    parts, picked = got[:, :, 0], got[:, :, 1]
    top = jnp.max(parts, axis=0)
    return top + jnp.log(jnp.sum(jnp.exp(parts - top[None]), axis=0)) - jnp.sum(picked, axis=0)


def solution(mesh):
    return jax.shard_map(
        local,
        mesh=mesh,
        in_specs=(P(("dp", "vocab"), None), P("dp"), P("dp", None), P(None, "vocab")),
        out_specs=P(("dp", "vocab"), None),
        check_vma=False,
    )
```

```python
import functools
import math

import jax
import jax.numpy as jnp
from jax import lax
from jax.experimental import pallas as pl
from jax.experimental.pallas import tpu as pltpu
from jax.sharding import PartitionSpec as P

LOG2E = math.log2(math.e)
FLOOR = -1e30


def tree(op, values):
    while len(values) > 1:
        paired = [op(a, b) for a, b in zip(values[::2], values[1::2])]
        values = paired + ([values[-1]] if len(values) % 2 else [])
    return values[0]


def head_kernel(*refs, pieces, chunk, width, group, length):
    parts, (lab_ref, slot_ref, w_ref, o_ref, m_ref, s_ref, p_ref, lb_ref, x_ref, xt_ref) = refs[:pieces], refs[pieces:]
    tokens = x_ref.shape[0]
    block = w_ref.shape[0]
    step, steps = pl.program_id(0), pl.num_programs(0)

    def labels():
        value = lab_ref[...]
        return jnp.where((value >= 0) & (value < width), value, -(1 << 30))

    @pl.when(step == 0)
    def _():
        at = 0
        for part in parts:
            x_ref[at : at + part.shape[0], :] = part[...]
            at += part.shape[0]
        lb_ref[...] = jnp.broadcast_to(jnp.right_shift(labels(), 3), lb_ref.shape)
        m_ref[...] = jnp.full_like(m_ref, FLOOR)
        s_ref[...] = jnp.zeros_like(s_ref)
        p_ref[...] = jnp.zeros_like(p_ref)
        xt_ref[...] = x_ref[...].T

    sub = lax.broadcasted_iota(jnp.int32, (8, 128), 0)

    def run(masked):
        for r0 in range(0, block, chunk):
            logits = jnp.dot(w_ref[r0 : r0 + chunk, :], xt_ref[...], preferred_element_type=jnp.float32)
            for c in range(tokens // 128):
                cols = slice(c * 128, (c + 1) * 128)
                pick, top, total = p_ref[:, cols], m_ref[:, cols], s_ref[:, cols]
                label = lb_ref[:, cols] - (step * (block // 8) + r0 // 8)
                for g in range(0, chunk, group):
                    values = []
                    for r in range(g, min(g + group, chunk), 8):
                        value = logits[r : r + 8, cols]
                        if masked:
                            value = jnp.where(sub + (step * block + r0 + r) < width, value, FLOOR)
                        pick = jnp.where(label == r // 8, value, pick)
                        values.append(value)
                    peak = jnp.maximum(top, tree(jnp.maximum, values))
                    fresh = tree(jnp.add, [jnp.exp2((v - peak) * LOG2E) for v in values])
                    total = total * jnp.exp2((top - peak) * LOG2E) + fresh
                    top = peak
                p_ref[:, cols], m_ref[:, cols], s_ref[:, cols] = pick, top, total

    @pl.when(step < steps - 1)
    def _():
        run(False)

    @pl.when(step == steps - 1)
    def _():
        run(width % block != 0)
        top = m_ref[...]
        peak = jnp.max(top, axis=0, keepdims=True)
        total = jnp.sum(s_ref[...] * jnp.exp2((top - peak) * LOG2E), axis=0, keepdims=True)
        lse = peak + jnp.log(total)
        eight = lax.broadcasted_iota(jnp.int32, p_ref.shape, 0)
        picked = jnp.sum(jnp.where((labels() & 7) == eight, p_ref[...], 0.0), axis=0, keepdims=True)
        slots = o_ref.shape[0]
        mine = lax.broadcasted_iota(jnp.int32, (slots, tokens), 0) == slot_ref[...]
        token = lax.broadcasted_iota(jnp.int32, (tokens, length), 0)
        lane = lax.broadcasted_iota(jnp.int32, (tokens, length), 1)
        spread = (lax.rem(token, length) == lane).astype(jnp.float32)
        for k, row in enumerate((lse, picked)):
            o_ref[:, k * length : (k + 1) * length] = jnp.dot(
                jnp.where(mine, row, 0.0), spread, precision=lax.Precision.HIGHEST, preferred_element_type=jnp.float32
            )


def head_stats(parts, labels, slots, rows, slot_count, length):
    tokens, depth = labels.shape[1], rows.shape[1]
    width = rows.shape[0]
    block, chunk = 3168, 144
    return pl.pallas_call(
        functools.partial(head_kernel, pieces=len(parts), chunk=chunk, width=width, group=24, length=length),
        out_shape=jax.ShapeDtypeStruct((slot_count, 2 * length), jnp.float32),
        grid=(pl.cdiv(width, block),),
        in_specs=[pl.BlockSpec(part.shape, lambda j: (0, 0)) for part in parts]
        + [
            pl.BlockSpec((1, tokens), lambda j: (0, 0)),
            pl.BlockSpec((1, tokens), lambda j: (0, 0)),
            pl.BlockSpec((block, depth), lambda j: (j, 0)),
        ],
        out_specs=pl.BlockSpec((slot_count, 2 * length), lambda j: (0, 0)),
        scratch_shapes=[pltpu.VMEM((8, tokens), jnp.float32)] * 3
        + [
            pltpu.VMEM((8, tokens), jnp.int32),
            pltpu.VMEM((tokens, depth), parts[0].dtype),
            pltpu.VMEM((depth, tokens), parts[0].dtype),
        ],
        compiler_params=pltpu.CompilerParams(vmem_limit_bytes=60 << 20),
    )(*parts, labels, slots, rows)


def combine_kernel(got_ref, o_ref):
    length = o_ref.shape[1]
    parts, picked = got_ref[:, :, :length], got_ref[:, :, length:]
    top = jnp.max(parts, axis=0)
    o_ref[...] = top + jnp.log(jnp.sum(jnp.exp(parts - top[None]), axis=0)) - jnp.sum(picked, axis=0)


def local(hidden, target_ids, owner, head):
    shards, me = lax.axis_size("vocab"), lax.axis_index("vocab")
    width = head.shape[1]
    count = hidden.shape[0]
    seq_group = owner.shape[1]
    own_count = seq_group // shards
    length = target_ids.shape[0] // seq_group

    def swap(v, k):
        return lax.ppermute(v, "vocab", [(i, i ^ k) for i in range(shards)])

    places = list(range(0, shards, 2)) + list(range(1, shards, 2))
    even = [hidden] + [swap(hidden, k) for k in range(2, shards, 2)]
    parts = even + [swap(v, 1) for v in even]
    per_shard = count // length
    labels = jnp.concatenate([lax.dynamic_slice_in_dim(target_ids, (me ^ k) * count, count) for k in places])
    slots = jnp.concatenate([lax.dynamic_slice_in_dim(owner[0], (me ^ k) * per_shard, per_shard) for k in places])
    slots = jnp.broadcast_to(slots[:, None], (seq_group, length)).reshape(1, seq_group * length)
    send = head_stats(parts, (labels - me * width)[None, :], slots, head.T, seq_group, length)
    got = lax.all_to_all(send, "vocab", split_axis=0, concat_axis=0, tiled=True)
    return pl.pallas_call(combine_kernel, out_shape=jax.ShapeDtypeStruct((own_count, length), jnp.float32))(
        got.reshape(shards, own_count, 2 * length)
    )


def solution(mesh):
    return jax.shard_map(
        local,
        mesh=mesh,
        in_specs=(P(("dp", "vocab"), None), P("dp"), P("dp", None), P(None, "vocab")),
        out_specs=P(("dp", "vocab"), None),
        check_vma=False,
    )
```

```python
import functools
import math

import jax
import jax.numpy as jnp
from jax import lax
from jax.experimental import pallas as pl
from jax.experimental.pallas import tpu as pltpu
from jax.sharding import PartitionSpec as P

LOG2E = math.log2(math.e)
FLOOR = -1e30


def tree(op, values):
    while len(values) > 1:
        paired = [op(a, b) for a, b in zip(values[::2], values[1::2])]
        values = paired + ([values[-1]] if len(values) % 2 else [])
    return values[0]


def head_kernel(*refs, pieces, block, chunk, pull, width, group, length, shards):
    parts = refs[:pieces]
    lab_any, slot_any, w_any, o_ref = refs[pieces : pieces + 4]
    m_ref, s_ref, p_ref, lb_ref, lab_ref, slot_ref, x_ref, xt_ref, w_ref, sems, head_sems = refs[pieces + 4 :]
    tokens = x_ref.shape[0]
    blocks = w_ref.shape[0] // block

    copies, at = [], 0
    for part in parts:
        copies.append((part, x_ref.at[pl.ds(at, part.shape[0]), :]))
        at += part.shape[0]
    copies += [(lab_any, lab_ref), (slot_any, slot_ref)]
    copies = [pltpu.make_async_copy(src, dst, sems.at[i]) for i, (src, dst) in enumerate(copies)]

    def head_copy(index, count):
        rows = pl.ds(pl.multiple_of(index * pull, 8), count)
        return pltpu.make_async_copy(w_any.at[rows, :], w_ref.at[rows, :], head_sems.at[index])

    counts = [min(pull, width - start) for start in range(0, width, pull)]
    for copy in copies:
        copy.start()
    for index, count in enumerate(counts):
        head_copy(index, count).start()

    def labels():
        value = lab_ref[...]
        return jnp.where((value >= 0) & (value < width), value, -(1 << 30))

    m_ref[...] = jnp.full_like(m_ref, FLOOR)
    s_ref[...] = jnp.zeros_like(s_ref)
    p_ref[...] = jnp.zeros_like(p_ref)
    for copy in copies:
        copy.wait()
    lb_ref[...] = jnp.broadcast_to(jnp.right_shift(labels(), 3), lb_ref.shape)
    xt_ref[...] = x_ref[...].T

    sub = lax.broadcasted_iota(jnp.int32, (8, 128), 0)

    def run(step, masked):
        for r0 in range(0, block, chunk):
            if r0 % pull == 0:
                index = step * (block // pull) + r0 // pull
                if not masked:
                    head_copy(index, pull).wait()
                elif index < len(counts):
                    head_copy(index, counts[index]).wait()
            rows = pl.ds(pl.multiple_of(step * block + r0, 16), chunk)
            logits = jnp.dot(w_ref[rows, :], xt_ref[...], preferred_element_type=jnp.float32)
            for c in range(tokens // 128):
                cols = slice(c * 128, (c + 1) * 128)
                pick, top, total = p_ref[:, cols], m_ref[:, cols], s_ref[:, cols]
                label = lb_ref[:, cols] - (step * (block // 8) + r0 // 8)
                for g in range(0, chunk, group):
                    values = []
                    for r in range(g, min(g + group, chunk), 8):
                        value = logits[r : r + 8, cols]
                        if masked:
                            value = jnp.where(sub + (step * block + r0 + r) < width, value, FLOOR)
                        pick = jnp.where(label == r // 8, value, pick)
                        values.append(value)
                    peak = jnp.maximum(top, tree(jnp.maximum, values))
                    fresh = tree(jnp.add, [jnp.exp2((v - peak) * LOG2E) for v in values])
                    total = total * jnp.exp2((top - peak) * LOG2E) + fresh
                    top = peak
                p_ref[:, cols], m_ref[:, cols], s_ref[:, cols] = pick, top, total

    def body(step, carry):
        run(step, False)
        return carry

    lax.fori_loop(0, blocks - 1, body, 0)
    run(blocks - 1, True)

    top = m_ref[...]
    peak = jnp.max(top, axis=0, keepdims=True)
    total = jnp.sum(s_ref[...] * jnp.exp2((top - peak) * LOG2E), axis=0, keepdims=True)
    lse = peak + jnp.log(total)
    eight = lax.broadcasted_iota(jnp.int32, p_ref.shape, 0)
    picked = jnp.sum(jnp.where((labels() & 7) == eight, p_ref[...], 0.0), axis=0, keepdims=True)
    per_shard = o_ref.shape[2] // (2 * length)
    first = lax.broadcasted_iota(jnp.int32, (shards, tokens), 0) * per_shard
    token = lax.broadcasted_iota(jnp.int32, (tokens, length), 0)
    lane = lax.broadcasted_iota(jnp.int32, (tokens, length), 1)
    spread = (lax.rem(token, length) == lane).astype(jnp.float32)
    for i in range(per_shard):
        mine = first + i == slot_ref[...]
        for k, row in enumerate((lse, picked)):
            placed = jnp.dot(
                jnp.where(mine, row, 0.0), spread, precision=lax.Precision.HIGHEST, preferred_element_type=jnp.float32
            )
            lanes = slice((2 * i + k) * length, (2 * i + k + 1) * length)
            for d in range(shards):
                o_ref[d, :, lanes] = placed[d : d + 1, :]


def head_stats(parts, labels, slots, rows, shards, per_shard, length):
    tokens = labels.shape[1]
    width, depth = rows.shape
    block, chunk, pull = 3168, 144, 1584
    blocks = pl.cdiv(width, block)
    return pl.pallas_call(
        functools.partial(
            head_kernel,
            pieces=len(parts),
            block=block,
            chunk=chunk,
            pull=pull,
            width=width,
            group=24,
            length=length,
            shards=shards,
        ),
        out_shape=jax.ShapeDtypeStruct((shards, 1, 2 * length * per_shard), jnp.float32),
        in_specs=[pl.BlockSpec(memory_space=pl.ANY)] * (len(parts) + 3),
        out_specs=pl.BlockSpec(memory_space=pltpu.VMEM),
        scratch_shapes=[pltpu.VMEM((8, tokens), jnp.float32)] * 3
        + [
            pltpu.VMEM((8, tokens), jnp.int32),
            pltpu.VMEM((1, tokens), jnp.int32),
            pltpu.VMEM((1, tokens), jnp.int32),
            pltpu.VMEM((tokens, depth), parts[0].dtype),
            pltpu.VMEM((depth, tokens), parts[0].dtype),
            pltpu.VMEM((blocks * block, depth), rows.dtype),
            pltpu.SemaphoreType.DMA((len(parts) + 2,)),
            pltpu.SemaphoreType.DMA((pl.cdiv(width, pull),)),
        ],
        compiler_params=pltpu.CompilerParams(vmem_limit_bytes=46 << 20),
    )(*parts, labels, slots, rows)


def combine_kernel(got_ref, o_ref):
    count, length = o_ref.shape
    got = got_ref[:, 0, :]
    top = jnp.max(got, axis=0, keepdims=True)
    lse = top + jnp.log(jnp.sum(jnp.exp(got - top), axis=0, keepdims=True))
    picked = jnp.sum(got, axis=0, keepdims=True)
    for i in range(count):
        at = 2 * i * length
        o_ref[i : i + 1, :] = lse[:, at : at + length] - picked[:, at + length : at + 2 * length]


def local(hidden, target_ids, owner, head):
    shards, me = lax.axis_size("vocab"), lax.axis_index("vocab")
    width = head.shape[1]
    count = hidden.shape[0]
    seq_group = owner.shape[1]
    own_count = seq_group // shards
    length = target_ids.shape[0] // seq_group

    def swap(v, k):
        return lax.ppermute(v, "vocab", [(i, i ^ k) for i in range(shards)])

    places = list(range(0, shards, 2)) + list(range(1, shards, 2))
    even = [hidden] + [swap(hidden, k) for k in range(2, shards, 2)]
    parts = even + [swap(v, 1) for v in even]
    per_shard = count // length
    labels = jnp.concatenate([lax.dynamic_slice_in_dim(target_ids, (me ^ k) * count, count) for k in places])
    slots = jnp.concatenate([lax.dynamic_slice_in_dim(owner[0], (me ^ k) * per_shard, per_shard) for k in places])
    slots = jnp.broadcast_to(slots[:, None], (seq_group, length)).reshape(1, seq_group * length)
    labels = (labels - me * width)[None, :]
    send = head_stats(parts, labels, slots, head.T, shards, own_count, length)
    got = lax.all_to_all(send, "vocab", split_axis=0, concat_axis=0, tiled=True)
    return pl.pallas_call(combine_kernel, out_shape=jax.ShapeDtypeStruct((own_count, length), jnp.float32))(got)


def solution(mesh):
    return jax.shard_map(
        local,
        mesh=mesh,
        in_specs=(P(("dp", "vocab"), None), P("dp"), P("dp", None), P(None, "vocab")),
        out_specs=P(("dp", "vocab"), None),
        check_vma=False,
    )
```

```python
import functools
import math

import jax
import jax.numpy as jnp
from jax import lax
from jax.experimental import pallas as pl
from jax.experimental.pallas import tpu as pltpu
from jax.sharding import PartitionSpec as P

LOG2E = math.log2(math.e)
FLOOR = -1e30


def tree(op, values):
    while len(values) > 1:
        paired = [op(a, b) for a, b in zip(values[::2], values[1::2])]
        values = paired + ([values[-1]] if len(values) % 2 else [])
    return values[0]


def head_kernel(*refs, pieces, chunk, width, group, length, shards):
    parts, (lab_ref, slot_ref, w_ref, o_ref, m_ref, s_ref, p_ref, lb_ref, x_ref, xt_ref) = refs[:pieces], refs[pieces:]
    tokens = x_ref.shape[0]
    block = w_ref.shape[0]
    step, steps = pl.program_id(0), pl.num_programs(0)

    def labels():
        value = lab_ref[...]
        return jnp.where((value >= 0) & (value < width), value, -(1 << 30))

    @pl.when(step == 0)
    def _():
        at = 0
        for part in parts:
            x_ref[at : at + part.shape[0], :] = part[...]
            at += part.shape[0]
        lb_ref[...] = jnp.broadcast_to(jnp.right_shift(labels(), 3), lb_ref.shape)
        m_ref[...] = jnp.full_like(m_ref, FLOOR)
        s_ref[...] = jnp.zeros_like(s_ref)
        p_ref[...] = jnp.zeros_like(p_ref)
        xt_ref[...] = x_ref[...].T

    sub = lax.broadcasted_iota(jnp.int32, (8, 128), 0)

    def run(masked):
        for r0 in range(0, block, chunk):
            logits = jnp.dot(w_ref[r0 : r0 + chunk, :], xt_ref[...], preferred_element_type=jnp.float32)
            for c in range(tokens // 128):
                cols = slice(c * 128, (c + 1) * 128)
                pick, top, total = p_ref[:, cols], m_ref[:, cols], s_ref[:, cols]
                label = lb_ref[:, cols] - (step * (block // 8) + r0 // 8)
                for g in range(0, chunk, group):
                    values = []
                    for r in range(g, min(g + group, chunk), 8):
                        value = logits[r : r + 8, cols]
                        if masked:
                            value = jnp.where(sub + (step * block + r0 + r) < width, value, FLOOR)
                        pick = jnp.where(label == r // 8, value, pick)
                        values.append(value)
                    peak = jnp.maximum(top, tree(jnp.maximum, values))
                    fresh = tree(jnp.add, [jnp.exp2((v - peak) * LOG2E) for v in values])
                    total = total * jnp.exp2((top - peak) * LOG2E) + fresh
                    top = peak
                p_ref[:, cols], m_ref[:, cols], s_ref[:, cols] = pick, top, total

    @pl.when(step < steps - 1)
    def _():
        run(False)

    @pl.when(step == steps - 1)
    def _():
        run(width % block != 0)
        top = m_ref[...]
        peak = jnp.max(top, axis=0, keepdims=True)
        total = jnp.sum(s_ref[...] * jnp.exp2((top - peak) * LOG2E), axis=0, keepdims=True)
        lse = peak + jnp.log(total)
        eight = lax.broadcasted_iota(jnp.int32, p_ref.shape, 0)
        picked = jnp.sum(jnp.where((labels() & 7) == eight, p_ref[...], 0.0), axis=0, keepdims=True)
        per_shard = o_ref.shape[2] // (2 * length)
        first = lax.broadcasted_iota(jnp.int32, (shards, tokens), 0) * per_shard
        token = lax.broadcasted_iota(jnp.int32, (tokens, length), 0)
        lane = lax.broadcasted_iota(jnp.int32, (tokens, length), 1)
        spread = (lax.rem(token, length) == lane).astype(jnp.float32)
        for i in range(per_shard):
            mine = first + i == slot_ref[...]
            for k, row in enumerate((lse, picked)):
                placed = jnp.dot(
                    jnp.where(mine, row, 0.0), spread, precision=lax.Precision.HIGHEST, preferred_element_type=jnp.float32
                )
                lanes = slice((2 * i + k) * length, (2 * i + k + 1) * length)
                for d in range(shards):
                    o_ref[d, :, lanes] = placed[d : d + 1, :]


def head_stats(parts, labels, slots, rows, shards, per_shard, length):
    tokens, depth = labels.shape[1], rows.shape[1]
    width = rows.shape[0]
    block, chunk = 3168, 144
    return pl.pallas_call(
        functools.partial(head_kernel, pieces=len(parts), chunk=chunk, width=width, group=24, length=length, shards=shards),
        out_shape=jax.ShapeDtypeStruct((shards, 1, 2 * length * per_shard), jnp.float32),
        grid=(pl.cdiv(width, block),),
        in_specs=[pl.BlockSpec(part.shape, lambda j: (0, 0)) for part in parts]
        + [
            pl.BlockSpec((1, tokens), lambda j: (0, 0)),
            pl.BlockSpec((1, tokens), lambda j: (0, 0)),
            pl.BlockSpec((block, depth), lambda j: (j, 0)),
        ],
        out_specs=pl.BlockSpec((shards, 1, 2 * length * per_shard), lambda j: (0, 0, 0)),
        scratch_shapes=[pltpu.VMEM((8, tokens), jnp.float32)] * 3
        + [
            pltpu.VMEM((8, tokens), jnp.int32),
            pltpu.VMEM((tokens, depth), parts[0].dtype),
            pltpu.VMEM((depth, tokens), parts[0].dtype),
        ],
        compiler_params=pltpu.CompilerParams(vmem_limit_bytes=40 << 20),
    )(*parts, labels, slots, rows)


def combine_kernel(got_ref, o_ref):
    count, length = o_ref.shape
    got = got_ref[:, 0, :]
    top = jnp.max(got, axis=0, keepdims=True)
    lse = top + jnp.log(jnp.sum(jnp.exp(got - top), axis=0, keepdims=True))
    picked = jnp.sum(got, axis=0, keepdims=True)
    for i in range(count):
        at = 2 * i * length
        o_ref[i : i + 1, :] = lse[:, at : at + length] - picked[:, at + length : at + 2 * length]


def local(hidden, target_ids, owner, head):
    shards, me = lax.axis_size("vocab"), lax.axis_index("vocab")
    width = head.shape[1]
    count = hidden.shape[0]
    seq_group = owner.shape[1]
    own_count = seq_group // shards
    length = target_ids.shape[0] // seq_group

    def swap(v, k):
        return lax.ppermute(v, "vocab", [(i, i ^ k) for i in range(shards)])

    places = list(range(0, shards, 2)) + list(range(1, shards, 2))
    even = [hidden] + [swap(hidden, k) for k in range(2, shards, 2)]
    parts = even + [swap(v, 1) for v in even]
    per_shard = count // length
    labels = jnp.concatenate([lax.dynamic_slice_in_dim(target_ids, (me ^ k) * count, count) for k in places])
    slots = jnp.concatenate([lax.dynamic_slice_in_dim(owner[0], (me ^ k) * per_shard, per_shard) for k in places])
    slots = jnp.broadcast_to(slots[:, None], (seq_group, length)).reshape(1, seq_group * length)
    labels = (labels - me * width)[None, :]
    send = head_stats(parts, labels, slots, head.T, shards, own_count, length)
    got = lax.all_to_all(send, "vocab", split_axis=0, concat_axis=0, tiled=True)
    return pl.pallas_call(combine_kernel, out_shape=jax.ShapeDtypeStruct((own_count, length), jnp.float32))(got)


def solution(mesh):
    return jax.shard_map(
        local,
        mesh=mesh,
        in_specs=(P(("dp", "vocab"), None), P("dp"), P("dp", None), P(None, "vocab")),
        out_specs=P(("dp", "vocab"), None),
        check_vma=False,
    )
```
